768 devices in a mesh: grp: 24 (over x, z_hi, core), bn: 32 (over z_lo, y).
Axes of the slice: x: 4, y: 8, z: 12 (z_hi: 3, z_lo: 4; z = z_hi * 4 + z_lo), core: 2. Of those that a mesh axis runs over, the one named last changes fastest.
Arguments:
- images: bfloat16 [96, 128, 64, 1024], P('grp', 'bn'), parts along dimension 0, may hold values from -64 to 64
- w_reduce: bfloat16 [1024, 256], replicated, may hold values from -0.1875 to 0.1875
- w_spatial: bfloat16 [3, 3, 256, 256], replicated, may hold values from -0.125 to 0.125
- w_expand: bfloat16 [256, 1024], replicated, may hold values from -0.375 to 0.375
- gain_first: float32 [256], replicated, may hold values from 0.25 to 1.75
- shift_first: float32 [256], replicated, may hold values from -3 to 3
- gain_middle: float32 [256], replicated, may hold values from 0.25 to 1.75
- shift_middle: float32 [256], replicated, may hold values from -3 to 3
- gain_last: float32 [1024], replicated, may hold values from 0.25 to 1.75
- shift_last: float32 [1024], replicated, may hold values from -3 to 3
Outputs:
- block_out: bfloat16 [96, 128, 64, 1024], P('grp', 'bn'), parts along dimension 0
The draws below stay inside these ranges and needn't reach their ends.
There are 24 independent parts, one for each index of `grp`. The reference program is written for one: setup_inputs(seed, part) draws one part's arguments, and reference() takes and returns one part's arrays. A program takes and returns all parts, laid end to end along the dimension named above; an argument that names none is the same for every part. Nothing has to cross between parts.
All inputs are finite; a program needn't handle non-finite values.
Results may differ from the reference program's by a relative error of at most 0.0034.
Values may be sent and summed in bfloat16 or wider, within the bound.
No kernel may reach another device: no remote copies, remote signals or barrier semaphores. Data moves between devices by JAX's collectives and lax.ppermute only.
A program may use at most 32 MiB of HBM per device.

```python
import math
import jax
import jax.numpy as jnp
from jax import lax

CH = 1024
MID = 256
IMGS = 4
WID = 64
HGT = 128


def draw_images(key, part):
    keys = jax.random.split(key, 8)
    noise = jnp.clip(jax.random.normal(keys[0], (IMGS, HGT, WID, CH), jnp.float32), -4.0, 4.0)
    position = jnp.arange(HGT, dtype=jnp.float32) / max(HGT - 1, 1)
    jitter = jnp.exp(jax.random.uniform(keys[1], (IMGS, HGT), jnp.float32, 0.0, math.log(1.5)))
    offset = 0.5 * jnp.clip(jax.random.normal(keys[2], (IMGS, CH), jnp.float32), -3.0, 3.0)
    scale = jnp.power(3.0, position)[None, :] * jitter
    row_freq = jax.random.randint(keys[4], (IMGS, 3), 0, 2).astype(jnp.float32)
    col_freq = jax.random.randint(keys[5], (IMGS, 3), 1, 3).astype(jnp.float32)
    phases = jax.random.uniform(keys[6], (IMGS, 3), jnp.float32, 0.0, 2.0 * math.pi)
    amplitude = jnp.clip(jax.random.normal(keys[7], (IMGS, 3), jnp.float32), -3.0, 3.0)
    rows = jnp.arange(HGT, dtype=jnp.float32) / HGT
    cols = jnp.arange(WID, dtype=jnp.float32) / WID
    angles = 2.0 * math.pi * (row_freq[:, :, None, None] * rows[None, None, :, None] + col_freq[:, :, None, None] * cols[None, None, None, :]) + phases[:, :, None, None]
    waves = jnp.sum(amplitude[:, :, None, None] * jnp.cos(angles), axis=1)
    field = jnp.exp(0.7 * jnp.tanh(waves))
    values = (noise + offset[:, None, None, :]) * (scale[:, :, None] * field)[:, :, :, None]
    return values.astype(jnp.bfloat16)


def scatter_about(key, extent, scale, reach, held_as=jnp.bfloat16):
    array = jax.random.normal(key, extent, jnp.float32) * scale
    return jnp.minimum(jnp.maximum(array, -reach), reach).astype(held_as)


def setup_inputs(seed: int = 0, part: int = 0) -> dict:
    seeds = jax.random.split(jax.random.key(seed), 11)
    part_splits = jax.random.split(jax.random.fold_in(seeds[10], part), 11)
    images = draw_images(jax.random.fold_in(jax.random.fold_in(seeds[10], part), 71), part)
    w_reduce = scatter_about(seeds[1], (CH, MID), CH ** -0.5, 0.1875)
    w_spatial = scatter_about(seeds[2], (3, 3, MID, MID), (9 * MID) ** -0.5, 0.125)
    w_expand = scatter_about(seeds[3], (MID, CH), MID ** -0.5, 0.375)
    gain_first = jnp.clip(1.0 + 0.15 * jax.random.normal(seeds[4], (MID,), jnp.float32), 0.25, 1.75)
    shift_first = scatter_about(seeds[5], (MID,), 0.5, 3.0, jnp.float32)
    gain_middle = jnp.clip(1.0 + 0.15 * jax.random.normal(seeds[6], (MID,), jnp.float32), 0.25, 1.75)
    shift_middle = scatter_about(seeds[7], (MID,), 0.5, 3.0, jnp.float32)
    gain_last = jnp.clip(1.0 + 0.15 * jax.random.normal(seeds[8], (CH,), jnp.float32), 0.25, 1.75)
    shift_last = scatter_about(seeds[9], (CH,), 0.5, 3.0, jnp.float32)
    return {"images": images, "w_reduce": w_reduce, "w_spatial": w_spatial, "w_expand": w_expand, "gain_first": gain_first, "shift_first": shift_first, "gain_middle": gain_middle, "shift_middle": shift_middle, "gain_last": gain_last, "shift_last": shift_last}


epsilon = 1e-05

def normalize(values, gain, shift):
    population = values.shape[0] * values.shape[1] * values.shape[2]
    average = lax.optimization_barrier(jnp.sum(values, axis=(0, 1, 2))) / population
    centred = values - average
    spread = lax.optimization_barrier(jnp.sum(centred * centred, axis=(0, 1, 2))) / population
    return centred * (gain * lax.rsqrt(spread + epsilon)) + shift

def pointwise(inputs, weight):
    flat = inputs.reshape(-1, inputs.shape[-1])
    product = jnp.dot(flat, weight, preferred_element_type=jnp.float32)
    return product.reshape(inputs.shape[:-1] + (weight.shape[1],))

def reference(images, w_reduce, w_spatial, w_expand, gain_first, shift_first, gain_middle, shift_middle, gain_last, shift_last):
    first = pointwise(images, w_reduce)
    hidden_first = jax.nn.relu(normalize(first, gain_first, shift_first)).astype(jnp.bfloat16)
    middle = lax.conv_general_dilated(hidden_first, w_spatial, (1, 1), 'SAME', dimension_numbers=('NHWC', 'HWIO', 'NHWC'), preferred_element_type=jnp.float32)
    hidden_middle = jax.nn.relu(normalize(middle, gain_middle, shift_middle)).astype(jnp.bfloat16)
    last = pointwise(hidden_middle, w_expand)
    return jax.nn.relu(normalize(last, gain_last, shift_last) + images.astype(jnp.float32)).astype(jnp.bfloat16)
```

```python
import jax
import jax.numpy as jnp
from jax import lax
from jax.experimental import pallas as pl
from jax.experimental.pallas import tpu as pltpu
from jax.sharding import PartitionSpec as P

epsilon = 1e-05
f32 = jnp.float32
bf16 = jnp.bfloat16

VM = pl.BlockSpec(memory_space=pltpu.VMEM)
SM = pl.BlockSpec(memory_space=pltpu.SMEM)
HB = pl.BlockSpec(memory_space=pltpu.HBM)


def in_vmem(value):
    return pltpu.with_memory_space_constraint(value, pltpu.VMEM)


def in_hbm(value):
    return pltpu.with_memory_space_constraint(value, pltpu.HBM)


def call(kernel, outs, in_specs, out_specs, scratch=(), flops=0):
    return pl.pallas_call(
        kernel,
        out_shape=outs,
        in_specs=in_specs,
        out_specs=out_specs,
        scratch_shapes=list(scratch),
        compiler_params=pltpu.CompilerParams(vmem_limit_bytes=16 << 20),
        cost_estimate=pl.CostEstimate(flops=flops, bytes_accessed=1 << 20, transcendentals=0),
    )


def eights(block):
    return jnp.sum(block.reshape(block.shape[0] // 8, 8, block.shape[1]), axis=0)


def store_sums(out, total, squares):
    out[0:1, :] = jnp.sum(total, axis=0, keepdims=True)
    out[1:2, :] = jnp.sum(squares, axis=0, keepdims=True)


def factors(gathered, gain, shift, population):
    sums = jnp.sum(gathered[...], axis=0)
    average = sums[0:1, :] / population
    spread = sums[1:2, :] / population - average * average
    return average, gain[...] * lax.rsqrt(spread + epsilon), shift[...]


def reduce_kernel(place, images, weight, first, near, far, sums, kept, w_vmem, sem):
    imgs, rows, wid, ch = images.shape
    copies = [pltpu.make_async_copy(weight, w_vmem, sem.at[imgs])]
    copies += [pltpu.make_async_copy(images.at[n], kept.at[n], sem.at[n]) for n in range(imgs)]
    for c in copies:
        c.start()
    for c in copies:
        c.wait()
    even = place[0] % 2 == 0
    total = squares = None
    for n in range(imgs):
        x = kept[n].reshape(rows * wid, ch)
        y = jnp.dot(x, w_vmem[...], preferred_element_type=f32)
        for r in range(rows):
            first[r, n * wid : (n + 1) * wid, :] = y[r * wid : (r + 1) * wid]
        head, tail = y[:wid].astype(bf16), y[(rows - 1) * wid :].astype(bf16)
        near[n * wid : (n + 1) * wid, :] = jnp.where(even, tail, head)
        far[n * wid : (n + 1) * wid, :] = jnp.where(even, head, tail)
        a, b = eights(y), eights(y * y)
        total, squares = (a, b) if n == 0 else (total + a, squares + b)
    store_sums(sums, total, squares)


def spread_columns(hidden, out, wid):
    count, c = hidden.shape
    column = lax.broadcasted_iota(jnp.int32, (count, 1), 0) % wid
    left = jnp.where(column == 0, 0.0, pltpu.roll(hidden, 1, 0))
    right = jnp.where(column == wid - 1, 0.0, pltpu.roll(hidden, count - 1, 0))
    out[:, 0:c] = left.astype(bf16)
    out[:, c : 2 * c] = hidden.astype(bf16)
    out[:, 2 * c : 3 * c] = right.astype(bf16)


def inner_kernel(wid, population, first, gathered, gain, shift, weight, mid, sums, norm, cells):
    rows = first.shape[0]
    average, factor, bias = factors(gathered, gain, shift, population)
    norm[0:1, :] = average
    norm[1:2, :] = factor
    norm[2:3, :] = bias
    for r in range(rows):
        hidden = jnp.maximum((first[r] - average) * factor + bias, 0.0)
        spread_columns(hidden, cells.at[r], wid)
    k = cells.shape[2]
    total = squares = None
    for r in range(rows):
        lo, hi = max(r - 1, 0), min(r + 2, rows)
        lhs = jnp.concatenate([cells[i] for i in range(lo, hi)], axis=1)
        y = jnp.dot(lhs, weight[(lo - r + 1) * k : (hi - r + 1) * k, :], preferred_element_type=f32)
        mid[r] = y
        if r > 0 and r < rows - 1:
            a, b = eights(y), eights(y * y)
            total, squares = (a, b) if total is None else (total + a, squares + b)
    sums[0] = total
    sums[1] = squares


def edge_kernel(wid, ends, place, mid, near, far, norm, weight, inner, edge, sums, cells):
    rows = mid.shape[0]
    k = cells.shape[2]
    even = place[0] % 2 == 0
    for i in range(2):
        halo = jnp.where(even == (i == 0), far[...], near[...]).astype(f32)
        hidden = jnp.maximum((halo - norm[0:1, :]) * norm[1:2, :] + norm[2:3, :], 0.0)
        hidden = jnp.where(place[0] == (0 if i == 0 else ends), 0.0, hidden)
        spread_columns(hidden, cells.at[i], wid)
    total, squares = inner[0], inner[1]
    for i in range(2):
        y = mid[(rows - 1) * i] + jnp.dot(
            cells[i], weight[2 * i * k : (2 * i + 1) * k, :], preferred_element_type=f32
        )
        edge[i] = y
        total, squares = total + eights(y), squares + eights(y * y)
    store_sums(sums, total, squares)


def expand_kernel(population, mid, edge, gathered, gain, shift, weight, last, sums):
    rows = mid.shape[0]
    average, factor, bias = factors(gathered, gain, shift, population)
    total = squares = None
    for r in range(rows):
        value = edge[0] if r == 0 else edge[1] if r == rows - 1 else mid[r]
        hidden = jnp.maximum((value - average) * factor + bias, 0.0).astype(bf16)
        y = jnp.dot(hidden, weight[...], preferred_element_type=f32)
        last[r] = y
        a, b = eights(y), eights(y * y)
        total, squares = (a, b) if r == 0 else (total + a, squares + b)
    store_sums(sums, total, squares)


def final_kernel(population, last, images, gathered, gain, shift, out, staged, sem):
    imgs, rows, wid, _ = images.shape
    average, factor, bias = factors(gathered, gain, shift, population)
    copies = []
    for n in range(imgs):
        for r in range(rows):
            value = (last[r, n * wid : (n + 1) * wid, :] - average) * factor + bias
            value = value + images[n, r].astype(f32)
            staged[n, r] = jnp.maximum(value, 0.0).astype(bf16)
            copies.append(pltpu.make_async_copy(staged.at[n, r], out.at[n, r], sem.at[n, r]))
            copies[-1].start()
    for c in copies:
        c.wait()


def pairs(start, count):
    firsts = range(start, count - 1, 2)
    return [(i, i + 1) for i in firsts] + [(i + 1, i) for i in firsts]


def to_all(sums, count):
    copies = jnp.broadcast_to(sums, (count, 1, *sums.shape))
    got = lax.all_to_all(copies, "bn", split_axis=0, concat_axis=0, tiled=True)
    return in_vmem(got.reshape(count, *sums.shape))


def body(
    images,
    w_reduce,
    w_spatial,
    w_expand,
    gain_first,
    shift_first,
    gain_middle,
    shift_middle,
    gain_last,
    shift_last,
):
    count = lax.axis_size("bn")
    imgs, rows, wid, ch = images.shape
    mid_ch = w_reduce.shape[1]
    cells = imgs * wid
    population = float(cells * rows * count)
    row = lambda v: in_vmem(v.reshape(1, -1))

    place = lax.axis_index("bn").astype(jnp.int32).reshape(1)
    first, near, far, sums = call(
        reduce_kernel,
        [
            pltpu.VMEM((rows, cells, mid_ch), f32),
            pltpu.VMEM((cells, mid_ch), bf16),
            pltpu.VMEM((cells, mid_ch), bf16),
            pltpu.VMEM((2, mid_ch), f32),
        ],
        [SM, HB, HB],
        [VM] * 4,
        [pltpu.VMEM(images.shape, bf16), pltpu.VMEM(w_reduce.shape, bf16), pltpu.SemaphoreType.DMA((imgs + 1,))],
        2 * cells * rows * ch * mid_ch,
    )(place, in_hbm(images), in_hbm(w_reduce))
    far = lax.ppermute(far, "bn", pairs(1, count))
    near = lax.ppermute(near, "bn", pairs(0, count))

    w_spatial, sums = lax.optimization_barrier((w_spatial, sums))
    gathered = to_all(sums, count)
    weight = in_vmem(w_spatial.reshape(-1, mid_ch))
    middle, inner, norm = call(
        lambda *refs: inner_kernel(wid, population, *refs),
        [
            pltpu.VMEM((rows, cells, mid_ch), f32),
            pltpu.VMEM((2, 8, mid_ch), f32),
            pltpu.VMEM((3, mid_ch), f32),
        ],
        [VM] * 5,
        [VM] * 3,
        [pltpu.VMEM((rows, cells, 3 * mid_ch), bf16)],
        2 * cells * rows * 9 * mid_ch * mid_ch,
    )(first, gathered, row(gain_first), row(shift_first), weight)
    edge, sums = call(
        lambda *refs: edge_kernel(wid, count - 1, *refs),
        [pltpu.VMEM((2, cells, mid_ch), f32), pltpu.VMEM((2, mid_ch), f32)],
        [SM] + [VM] * 6,
        [VM] * 2,
        [pltpu.VMEM((2, cells, 3 * mid_ch), bf16)],
        2 * cells * 6 * mid_ch * mid_ch,
    )(place, middle, in_vmem(near), in_vmem(far), norm, weight, inner)
    images, w_expand, sums = lax.optimization_barrier((images, w_expand, sums))
    gathered = to_all(sums, count)

    last, sums = call(
        lambda *refs: expand_kernel(population, *refs),
        [pltpu.VMEM((rows, cells, ch), f32), pltpu.VMEM((2, ch), f32)],
        [VM] * 6,
        [VM] * 2,
        (),
        2 * cells * rows * ch * mid_ch,
    )(middle, edge, gathered, row(gain_middle), row(shift_middle), in_vmem(w_expand))
    gathered = to_all(sums, count)

    return call(
        lambda *refs: final_kernel(population, *refs),
        jax.ShapeDtypeStruct(images.shape, bf16),
        [VM] * 5,
        HB,
        [pltpu.VMEM(images.shape, bf16), pltpu.SemaphoreType.DMA((imgs, rows))],
        8 * cells * rows * ch,
    )(last, in_vmem(images), gathered, row(gain_last), row(shift_last))


def solution(mesh):
    placed = (P("grp", "bn", None, None), P(), P(), P(), P(), P(), P(), P(), P(), P())
    return jax.shard_map(
        body, mesh=mesh, in_specs=placed, out_specs=P("grp", "bn", None, None), check_vma=False
    )
```

```python
import jax
import jax.numpy as jnp
from jax import lax
from jax.experimental import pallas as pl
from jax.experimental.pallas import tpu as pltpu
from jax.sharding import PartitionSpec as P

epsilon = 1e-05
LEADS0 = (4, 5, 5)
LEADS = (5, 5, 5)
f32 = jnp.float32
bf16 = jnp.bfloat16

VM = pl.BlockSpec(memory_space=pltpu.VMEM)
SM = pl.BlockSpec(memory_space=pltpu.SMEM)
HB = pl.BlockSpec(memory_space=pltpu.HBM)


def in_vmem(value):
    return pltpu.with_memory_space_constraint(value, pltpu.VMEM)


def in_hbm(value):
    return pltpu.with_memory_space_constraint(value, pltpu.HBM)


def call(kernel, outs, in_specs, out_specs, scratch=(), flops=0):
    return pl.pallas_call(
        kernel,
        out_shape=outs,
        in_specs=in_specs,
        out_specs=out_specs,
        scratch_shapes=list(scratch),
        compiler_params=pltpu.CompilerParams(vmem_limit_bytes=16 << 20),
        cost_estimate=pl.CostEstimate(flops=flops, bytes_accessed=1 << 20, transcendentals=0),
    )


def eights(block):
    return jnp.sum(block.reshape(block.shape[0] // 8, 8, block.shape[1]), axis=0)


def store_sums(out, total, squares):
    out[0:1, :] = jnp.sum(total, axis=0, keepdims=True)
    out[1:2, :] = jnp.sum(squares, axis=0, keepdims=True)


def factors(gathered, gain, shift, population):
    sums = jnp.sum(gathered[...], axis=0)
    average = sums[0:1, :] / population
    spread = sums[1:2, :] / population - average * average
    return average, gain[...] * lax.rsqrt(spread + epsilon), shift[...]


def reduce_kernel(place, images, weight, first, near, far, sums, kept, w_vmem, sem):
    imgs, rows, wid, ch = images.shape
    copies = [pltpu.make_async_copy(weight, w_vmem, sem.at[imgs])]
    copies += [pltpu.make_async_copy(images.at[n], kept.at[n], sem.at[n]) for n in range(imgs)]
    for c in copies:
        c.start()
    for c in copies:
        c.wait()
    even = place[0] % 2 == 0
    total = squares = None
    for n in range(imgs):
        x = kept[n].reshape(rows * wid, ch)
        y = jnp.dot(x, w_vmem[...], preferred_element_type=f32)
        for r in range(rows):
            first[r, n * wid : (n + 1) * wid, :] = y[r * wid : (r + 1) * wid]
        head, tail = y[:wid].astype(bf16), y[(rows - 1) * wid :].astype(bf16)
        near[n * wid : (n + 1) * wid, :] = jnp.where(even, tail, head)
        far[n * wid : (n + 1) * wid, :] = jnp.where(even, head, tail)
        a, b = eights(y), eights(y * y)
        total, squares = (a, b) if n == 0 else (total + a, squares + b)
    store_sums(sums, total, squares)


def spread_columns(hidden, out, wid):
    count, c = hidden.shape
    column = lax.broadcasted_iota(jnp.int32, (count, 1), 0) % wid
    left = jnp.where(column == 0, 0.0, pltpu.roll(hidden, 1, 0))
    right = jnp.where(column == wid - 1, 0.0, pltpu.roll(hidden, count - 1, 0))
    out[:, 0:c] = left.astype(bf16)
    out[:, c : 2 * c] = hidden.astype(bf16)
    out[:, 2 * c : 3 * c] = right.astype(bf16)


def inner_kernel(wid, population, first, gathered, gain, shift, weight, mid, sums, norm, cells):
    rows = first.shape[0]
    average, factor, bias = factors(gathered, gain, shift, population)
    norm[0:1, :] = average
    norm[1:2, :] = factor
    norm[2:3, :] = bias
    for r in range(rows):
        hidden = jnp.maximum((first[r] - average) * factor + bias, 0.0)
        spread_columns(hidden, cells.at[r], wid)
    k = cells.shape[2]
    total = squares = None
    for r in range(rows):
        lo, hi = max(r - 1, 0), min(r + 2, rows)
        lhs = jnp.concatenate([cells[i] for i in range(lo, hi)], axis=1)
        y = jnp.dot(lhs, weight[(lo - r + 1) * k : (hi - r + 1) * k, :], preferred_element_type=f32)
        mid[r] = y
        if r > 0 and r < rows - 1:
            a, b = eights(y), eights(y * y)
            total, squares = (a, b) if total is None else (total + a, squares + b)
    sums[0] = total
    sums[1] = squares


def edge_kernel(wid, ends, place, mid, near, far, norm, weight, inner, edge, sums, cells):
    rows = mid.shape[0]
    k = cells.shape[2]
    even = place[0] % 2 == 0
    for i in range(2):
        halo = jnp.where(even == (i == 0), far[...], near[...]).astype(f32)
        hidden = jnp.maximum((halo - norm[0:1, :]) * norm[1:2, :] + norm[2:3, :], 0.0)
        hidden = jnp.where(place[0] == (0 if i == 0 else ends), 0.0, hidden)
        spread_columns(hidden, cells.at[i], wid)
    total, squares = inner[0], inner[1]
    for i in range(2):
        y = mid[(rows - 1) * i] + jnp.dot(
            cells[i], weight[2 * i * k : (2 * i + 1) * k, :], preferred_element_type=f32
        )
        edge[i] = y
        total, squares = total + eights(y), squares + eights(y * y)
    store_sums(sums, total, squares)


def expand_kernel(population, mid, edge, gathered, gain, shift, weight, last, sums):
    rows = mid.shape[0]
    average, factor, bias = factors(gathered, gain, shift, population)
    c = weight.shape[0]
    total = squares = None
    for r in range(rows):
        value = edge[0] if r == 0 else edge[1] if r == rows - 1 else mid[r]
        hidden = jnp.maximum((value - average) * factor + bias, 0.0).astype(bf16)
        y = jnp.dot(hidden, weight[...], preferred_element_type=f32)
        last[r] = y
        a, b = eights(hidden.astype(f32)), eights(y * y)
        total, squares = (a, b) if r == 0 else (total + a, squares + b)
    squares = jnp.sum(squares, axis=0, keepdims=True)
    half = sums.shape[1]
    sums[0:1, 0:c] = jnp.sum(total, axis=0, keepdims=True)
    sums[0:1, c:half] = squares[:, : half - c]
    sums[1:2, :] = squares[:, half - c :]


def times(row, weight):
    high = row.astype(bf16).astype(f32)
    mid = (row - high).astype(bf16).astype(f32)
    low = (row - high - mid).astype(bf16).astype(f32)
    place = lax.broadcasted_iota(jnp.int32, (8, row.shape[1]), 0)
    pieces = jnp.where(place == 0, high, jnp.where(place == 1, mid, jnp.where(place == 2, low, 0.0)))
    product = jnp.dot(pieces.astype(bf16), weight, preferred_element_type=f32)
    return jnp.sum(product, axis=0, keepdims=True)


def final_kernel(population, last, images, gathered, gain, shift, weight, out, staged, sem):
    imgs, rows, wid, _ = images.shape
    c = weight.shape[0]
    sums = jnp.sum(gathered[...], axis=0)
    average = times(sums[0:1, :c] / population, weight[...])
    squares = jnp.concatenate([sums[0:1, c:], sums[1:2, :]], axis=1)
    spread = squares / population - average * average
    factor = gain[...] * lax.rsqrt(spread + epsilon)
    bias = shift[...] - average * factor
    copies = []
    for n in range(imgs):
        for r in range(rows):
            value = last[r, n * wid : (n + 1) * wid, :] * factor + bias
            value = value + images[n, r].astype(f32)
            staged[n, r] = jnp.maximum(value, 0.0).astype(bf16)
            copies.append(pltpu.make_async_copy(staged.at[n, r], out.at[n, r], sem.at[n, r]))
            copies[-1].start()
    for c in copies:
        c.wait()


def pairs(start, count):
    firsts = range(start, count - 1, 2)
    return [(i, i + 1) for i in firsts] + [(i + 1, i) for i in firsts]


def to_all(sums, heads):
    count = lax.axis_size("bn")
    groups = [
        [g * count + i for i in [head] + [i for i in range(count) if i != head]]
        for g, head in enumerate(heads)
    ]
    copies = jnp.broadcast_to(sums, (count, 1, *sums.shape))
    got = lax.all_to_all(
        copies, ("grp", "bn"), split_axis=0, concat_axis=0, tiled=True, axis_index_groups=groups
    )
    return in_vmem(got.reshape(count, *sums.shape))


def body(
    images,
    w_reduce,
    w_spatial,
    w_expand,
    gain_first,
    shift_first,
    gain_middle,
    shift_middle,
    gain_last,
    shift_last,
):
    count = lax.axis_size("bn")
    imgs, rows, wid, ch = images.shape
    mid_ch = w_reduce.shape[1]
    cells = imgs * wid
    eighth = count // 8
    heads = lambda i: [LEADS0[i - 1] * eighth] + [LEADS[i - 1] * eighth] * (lax.axis_size("grp") - 1)
    population = float(cells * rows * count)
    row = lambda v: in_vmem(v.reshape(1, -1))

    place = lax.axis_index("bn").astype(jnp.int32).reshape(1)
    first, near, far, sums = call(
        reduce_kernel,
        [
            pltpu.VMEM((rows, cells, mid_ch), f32),
            pltpu.VMEM((cells, mid_ch), bf16),
            pltpu.VMEM((cells, mid_ch), bf16),
            pltpu.VMEM((2, mid_ch), f32),
        ],
        [SM, HB, HB],
        [VM] * 4,
        [pltpu.VMEM(images.shape, bf16), pltpu.VMEM(w_reduce.shape, bf16), pltpu.SemaphoreType.DMA((imgs + 1,))],
        2 * cells * rows * ch * mid_ch,
    )(place, in_hbm(images), in_hbm(w_reduce))
    far = lax.ppermute(far, "bn", pairs(1, count))
    near = lax.ppermute(near, "bn", pairs(0, count))

    w_spatial, sums = lax.optimization_barrier((w_spatial, sums))
    gathered = to_all(sums, heads(1))
    weight = in_vmem(w_spatial.reshape(-1, mid_ch))
    middle, inner, norm = call(
        lambda *refs: inner_kernel(wid, population, *refs),
        [
            pltpu.VMEM((rows, cells, mid_ch), f32),
            pltpu.VMEM((2, 8, mid_ch), f32),
            pltpu.VMEM((3, mid_ch), f32),
        ],
        [VM] * 5,
        [VM] * 3,
        [pltpu.VMEM((rows, cells, 3 * mid_ch), bf16)],
        2 * cells * rows * 9 * mid_ch * mid_ch,
    )(first, gathered, row(gain_first), row(shift_first), weight)
    edge, sums = call(
        lambda *refs: edge_kernel(wid, count - 1, *refs),
        [pltpu.VMEM((2, cells, mid_ch), f32), pltpu.VMEM((2, mid_ch), f32)],
        [SM] + [VM] * 6,
        [VM] * 2,
        [pltpu.VMEM((2, cells, 3 * mid_ch), bf16)],
        2 * cells * 6 * mid_ch * mid_ch,
    )(place, middle, in_vmem(near), in_vmem(far), norm, weight, inner)
    images, w_expand, sums = lax.optimization_barrier((images, w_expand, sums))
    gathered = to_all(sums, heads(2))

    expand = in_vmem(w_expand)
    last, sums = call(
        lambda *refs: expand_kernel(population, *refs),
        [pltpu.VMEM((rows, cells, ch), f32), pltpu.VMEM((2, (mid_ch + ch) // 2), f32)],
        [VM] * 6,
        [VM] * 2,
        (),
        2 * cells * rows * ch * mid_ch,
    )(middle, edge, gathered, row(gain_middle), row(shift_middle), expand)
    gathered = to_all(sums, heads(3))

    return call(
        lambda *refs: final_kernel(population, *refs),
        jax.ShapeDtypeStruct(images.shape, bf16),
        [VM] * 6,
        HB,
        [pltpu.VMEM(images.shape, bf16), pltpu.SemaphoreType.DMA((imgs, rows))],
        8 * cells * rows * ch,
    )(last, in_vmem(images), gathered, row(gain_last), row(shift_last), expand)


def solution(mesh):
    placed = (P("grp", "bn", None, None), P(), P(), P(), P(), P(), P(), P(), P(), P())
    return jax.shard_map(
        body, mesh=mesh, in_specs=placed, out_specs=P("grp", "bn", None, None), check_vma=False
    )
```

```python
import jax
import jax.numpy as jnp
from jax import lax
from jax.experimental import pallas as pl
from jax.experimental.pallas import tpu as pltpu
from jax.sharding import PartitionSpec as P

epsilon = 1e-05
LEADS0 = (4, 5, 5)
LEADS = (5, 5, 5)
f32 = jnp.float32
bf16 = jnp.bfloat16

VM = pl.BlockSpec(memory_space=pltpu.VMEM)
SM = pl.BlockSpec(memory_space=pltpu.SMEM)
HB = pl.BlockSpec(memory_space=pltpu.HBM)


def in_vmem(value):
    return pltpu.with_memory_space_constraint(value, pltpu.VMEM)


def in_hbm(value):
    return pltpu.with_memory_space_constraint(value, pltpu.HBM)


def call(kernel, outs, in_specs, out_specs, scratch=(), flops=0):
    return pl.pallas_call(
        kernel,
        out_shape=outs,
        in_specs=in_specs,
        out_specs=out_specs,
        scratch_shapes=list(scratch),
        compiler_params=pltpu.CompilerParams(vmem_limit_bytes=16 << 20),
        cost_estimate=pl.CostEstimate(flops=flops, bytes_accessed=1 << 20, transcendentals=0),
    )


def eights(block):
    return jnp.sum(block.reshape(block.shape[0] // 8, 8, block.shape[1]), axis=0)


def store_sums(out, total, squares):
    out[0:1, :] = jnp.sum(total, axis=0, keepdims=True)
    out[1:2, :] = jnp.sum(squares, axis=0, keepdims=True)


def factors(gathered, gain, shift, population):
    sums = jnp.sum(gathered[...], axis=0)
    average = sums[0:1, :] / population
    spread = sums[1:2, :] / population - average * average
    return average, gain[...] * lax.rsqrt(spread + epsilon), shift[...]


def reduce_kernel(place, images, weight, first, near, far, sums, kept, w_vmem, sem):
    imgs, rows, wid, ch = images.shape
    copies = [pltpu.make_async_copy(weight, w_vmem, sem.at[imgs])]
    copies += [pltpu.make_async_copy(images.at[n], kept.at[n], sem.at[n]) for n in range(imgs)]
    for c in copies:
        c.start()
    for c in copies:
        c.wait()
    even = place[0] % 2 == 0
    total = squares = None
    for n in range(imgs):
        x = kept[n].reshape(rows * wid, ch)
        y = jnp.dot(x, w_vmem[...], preferred_element_type=f32)
        for r in range(rows):
            first[r, n * wid : (n + 1) * wid, :] = y[r * wid : (r + 1) * wid]
        a, b = eights(y), eights(y * y)
        total, squares = (a, b) if n == 0 else (total + a, squares + b)
    store_sums(sums, total, squares)
    own = sums[0:1, :] / float(imgs * rows * wid)
    head, tail = (first[0] - own).astype(bf16), (first[rows - 1] - own).astype(bf16)
    near[...] = jnp.where(even, tail, head)
    far[...] = jnp.where(even, head, tail)


def spread_columns(hidden, out, wid):
    count, c = hidden.shape
    column = lax.broadcasted_iota(jnp.int32, (count, 1), 0) % wid
    left = jnp.where(column == 0, 0.0, pltpu.roll(hidden, 1, 0))
    right = jnp.where(column == wid - 1, 0.0, pltpu.roll(hidden, count - 1, 0))
    out[:, 0:c] = left.astype(bf16)
    out[:, c : 2 * c] = hidden.astype(bf16)
    out[:, 2 * c : 3 * c] = right.astype(bf16)


def inner_kernel(wid, population, first, gathered, gain, shift, weight, mid, sums, norm, cells):
    rows = first.shape[0]
    average, factor, bias = factors(gathered, gain, shift, population)
    norm[0:1, :] = average
    norm[1:2, :] = factor
    norm[2:3, :] = bias
    for r in range(rows):
        hidden = jnp.maximum((first[r] - average) * factor + bias, 0.0)
        spread_columns(hidden, cells.at[r], wid)
    k = cells.shape[2]
    total = squares = None
    for r in range(rows):
        lo, hi = max(r - 1, 0), min(r + 2, rows)
        lhs = jnp.concatenate([cells[i] for i in range(lo, hi)], axis=1)
        y = jnp.dot(lhs, weight[(lo - r + 1) * k : (hi - r + 1) * k, :], preferred_element_type=f32)
        mid[r] = y
        if r > 0 and r < rows - 1:
            a, b = eights(y), eights(y * y)
            total, squares = (a, b) if total is None else (total + a, squares + b)
    sums[0] = total
    sums[1] = squares


def edge_kernel(wid, ends, heads, place, part, mid, near, far, gathered, norm, weight, inner, edge, sums, cells):
    rows = mid.shape[0]
    k = cells.shape[2]
    even = place[0] % 2 == 0
    leader = jnp.where(part[0] == 0, heads[0], heads[1])
    for i in range(2):
        sender = jnp.clip(place[0] + 2 * i - 1, 0, ends)
        slot = jnp.where(sender == leader, 0, jnp.where(sender < leader, sender + 1, sender))
        shift = gathered[pl.ds(slot, 1)][0, 0:1, :] / float(rows * mid.shape[1])
        halo = jnp.where(even == (i == 0), far[...], near[...]).astype(f32) + shift
        hidden = jnp.maximum((halo - norm[0:1, :]) * norm[1:2, :] + norm[2:3, :], 0.0)
        hidden = jnp.where(place[0] == (0 if i == 0 else ends), 0.0, hidden)
        spread_columns(hidden, cells.at[i], wid)
    total, squares = inner[0], inner[1]
    for i in range(2):
        y = mid[(rows - 1) * i] + jnp.dot(
            cells[i], weight[2 * i * k : (2 * i + 1) * k, :], preferred_element_type=f32
        )
        edge[i] = y
        total, squares = total + eights(y), squares + eights(y * y)
    store_sums(sums, total, squares)


def expand_kernel(population, mid, edge, gathered, gain, shift, weight, last, sums):
    rows = mid.shape[0]
    average, factor, bias = factors(gathered, gain, shift, population)
    c = weight.shape[0]
    total = squares = None
    for r in range(rows):
        value = edge[0] if r == 0 else edge[1] if r == rows - 1 else mid[r]
        hidden = jnp.maximum((value - average) * factor + bias, 0.0).astype(bf16)
        y = jnp.dot(hidden, weight[...], preferred_element_type=f32)
        last[r] = y
        a, b = eights(hidden.astype(f32)), eights(y * y)
        total, squares = (a, b) if r == 0 else (total + a, squares + b)
    squares = jnp.sum(squares, axis=0, keepdims=True)
    half = sums.shape[1]
    sums[0:1, 0:c] = jnp.sum(total, axis=0, keepdims=True)
    sums[0:1, c:half] = squares[:, : half - c]
    sums[1:2, :] = squares[:, half - c :]


def times(row, weight):
    high = row.astype(bf16).astype(f32)
    mid = (row - high).astype(bf16).astype(f32)
    low = (row - high - mid).astype(bf16).astype(f32)
    place = lax.broadcasted_iota(jnp.int32, (8, row.shape[1]), 0)
    pieces = jnp.where(place == 0, high, jnp.where(place == 1, mid, jnp.where(place == 2, low, 0.0)))
    product = jnp.dot(pieces.astype(bf16), weight, preferred_element_type=f32)
    return jnp.sum(product, axis=0, keepdims=True)


def final_kernel(population, last, images, gathered, gain, shift, weight, out, staged, sem):
    imgs, rows, wid, _ = images.shape
    c = weight.shape[0]
    sums = jnp.sum(gathered[...], axis=0)
    average = times(sums[0:1, :c] / population, weight[...])
    squares = jnp.concatenate([sums[0:1, c:], sums[1:2, :]], axis=1)
    spread = squares / population - average * average
    factor = gain[...] * lax.rsqrt(spread + epsilon)
    bias = shift[...] - average * factor
    copies = []
    for n in range(imgs):
        for r in range(rows):
            value = last[r, n * wid : (n + 1) * wid, :] * factor + bias
            value = value + images[n, r].astype(f32)
            staged[n, r] = jnp.maximum(value, 0.0).astype(bf16)
            copies.append(pltpu.make_async_copy(staged.at[n, r], out.at[n, r], sem.at[n, r]))
            copies[-1].start()
    for c in copies:
        c.wait()


def pairs(start, count):
    firsts = range(start, count - 1, 2)
    return [(i, i + 1) for i in firsts] + [(i + 1, i) for i in firsts]


def to_all(sums, heads):
    count = lax.axis_size("bn")
    groups = [
        [g * count + i for i in [head] + [i for i in range(count) if i != head]]
        for g, head in enumerate(heads)
    ]
    copies = jnp.broadcast_to(sums, (count, 1, *sums.shape))
    got = lax.all_to_all(
        copies, ("grp", "bn"), split_axis=0, concat_axis=0, tiled=True, axis_index_groups=groups
    )
    return in_vmem(got.reshape(count, *sums.shape))


def body(
    images,
    w_reduce,
    w_spatial,
    w_expand,
    gain_first,
    shift_first,
    gain_middle,
    shift_middle,
    gain_last,
    shift_last,
):
    count = lax.axis_size("bn")
    imgs, rows, wid, ch = images.shape
    mid_ch = w_reduce.shape[1]
    cells = imgs * wid
    eighth = count // 8
    heads = lambda i: [LEADS0[i - 1] * eighth] + [LEADS[i - 1] * eighth] * (lax.axis_size("grp") - 1)
    place, part = (lax.axis_index(a).astype(jnp.int32).reshape(1) for a in ("bn", "grp"))
    first_heads = heads(1)[0], heads(1)[-1]
    population = float(cells * rows * count)
    row = lambda v: in_vmem(v.reshape(1, -1))

    first, near, far, sums = call(
        reduce_kernel,
        [
            pltpu.VMEM((rows, cells, mid_ch), f32),
            pltpu.VMEM((cells, mid_ch), bf16),
            pltpu.VMEM((cells, mid_ch), bf16),
            pltpu.VMEM((2, mid_ch), f32),
        ],
        [SM, HB, HB],
        [VM] * 4,
        [pltpu.VMEM(images.shape, bf16), pltpu.VMEM(w_reduce.shape, bf16), pltpu.SemaphoreType.DMA((imgs + 1,))],
        2 * cells * rows * ch * mid_ch,
    )(place, in_hbm(images), in_hbm(w_reduce))
    far = lax.ppermute(far, "bn", pairs(1, count))
    near = lax.ppermute(near, "bn", pairs(0, count))

    w_spatial, sums = lax.optimization_barrier((w_spatial, sums))
    gathered = to_all(sums, heads(1))
    weight = in_vmem(w_spatial.reshape(-1, mid_ch))
    middle, inner, norm = call(
        lambda *refs: inner_kernel(wid, population, *refs),
        [
            pltpu.VMEM((rows, cells, mid_ch), f32),
            pltpu.VMEM((2, 8, mid_ch), f32),
            pltpu.VMEM((3, mid_ch), f32),
        ],
        [VM] * 5,
        [VM] * 3,
        [pltpu.VMEM((rows, cells, 3 * mid_ch), bf16)],
        2 * cells * rows * 9 * mid_ch * mid_ch,
    )(first, gathered, row(gain_first), row(shift_first), weight)
    edge, sums = call(
        lambda *refs: edge_kernel(wid, count - 1, first_heads, *refs),
        [pltpu.VMEM((2, cells, mid_ch), f32), pltpu.VMEM((2, mid_ch), f32)],
        [SM] * 2 + [VM] * 7,
        [VM] * 2,
        [pltpu.VMEM((2, cells, 3 * mid_ch), bf16)],
        2 * cells * 6 * mid_ch * mid_ch,
    )(place, part, middle, in_vmem(near), in_vmem(far), gathered, norm, weight, inner)
    images, w_expand, sums = lax.optimization_barrier((images, w_expand, sums))
    gathered = to_all(sums, heads(2))

    expand = in_vmem(w_expand)
    last, sums = call(
        lambda *refs: expand_kernel(population, *refs),
        [pltpu.VMEM((rows, cells, ch), f32), pltpu.VMEM((2, (mid_ch + ch) // 2), f32)],
        [VM] * 6,
        [VM] * 2,
        (),
        2 * cells * rows * ch * mid_ch,
    )(middle, edge, gathered, row(gain_middle), row(shift_middle), expand)
    gathered = to_all(sums, heads(3))

    return call(
        lambda *refs: final_kernel(population, *refs),
        jax.ShapeDtypeStruct(images.shape, bf16),
        [VM] * 6,
        HB,
        [pltpu.VMEM(images.shape, bf16), pltpu.SemaphoreType.DMA((imgs, rows))],
        8 * cells * rows * ch,
    )(last, in_vmem(images), gathered, row(gain_last), row(shift_last), expand)


def solution(mesh):
    placed = (P("grp", "bn", None, None), P(), P(), P(), P(), P(), P(), P(), P(), P())
    return jax.shard_map(
        body, mesh=mesh, in_specs=placed, out_specs=P("grp", "bn", None, None), check_vma=False
    )
```
